32 devices in a mesh: dp: 8 (over y, x, core), mp: 4 (over z).
Axes of the slice: x: 2, y: 2, z: 4, core: 2. Of those that a mesh axis runs over, the one named last changes fastest.
Arguments:
- feature_ids: int32 [8, 2048, 8], P('dp'), may hold values from 0 to 4095
- tables: bfloat16 [8, 4096, 128], P('dp'), may hold values from -5 to 5
- table_of_feature: int32 [8], replicated, may hold values from 0 to 7, each once
- cross_down: bfloat16 [2, 1024, 512], P(None, 'mp'), may hold values from -0.1875 to 0.1875
- cross_up: bfloat16 [2, 1024, 512], P(None, 'mp'), may hold values from -0.125 to 0.125
- cross_bias: float32 [2, 1024], P(None, 'mp'), may hold values from -3 to 3
- tower_weight: bfloat16 [1024, 2048], P('dp', 'mp'), may hold values from -0.1875 to 0.1875
- tower_bias: float32 [2048], P('mp'), may hold values from -3 to 3
Outputs:
- hidden: bfloat16 [2048, 2048], P('dp', 'mp')
The draws below stay inside these ranges and needn't reach their ends.
Inputs may be any that keep to these rules, and one draw needn't show every extreme that they name: `feature_ids`: each id indexes a row of its own table. `table_of_feature`: each table serves exactly one feature.
All inputs are finite; a program needn't handle non-finite values.
Results may differ from the reference program's by a relative error of at most 0.015.
Values may be sent and summed in bfloat16 or wider, within the bound.
No kernel may reach another device: no remote copies, remote signals or barrier semaphores. Data moves between devices by JAX's collectives and lax.ppermute only.
A program may use at most 64 MiB of HBM per device.

```python
import math
import jax
import jax.numpy as jnp
import numpy as np
from jax import lax

EMBED = 128
RANK = 512
HID = 2048
VOCAB = 4096
HOTS = 8
LAYERS = 2
FEATS = 8
WIDTH = 1024
BATCH = 2048


def touch_ends(result, key, smallest, top_value):
    dims = result.shape
    index_at = [jax.random.randint(jax.random.fold_in(key, axis), (), 0, dims[axis]) for axis in range(len(dims))]
    result = result.at[tuple(index_at)].set(smallest)
    longest = dims.index(max(dims))
    index_at[longest] = (index_at[longest] + 1) % dims[longest]
    return result.at[tuple(index_at)].set(top_value)


def block_scale(stream_key, dims, split, least, largest):
    gain = 1.0
    for position, parts in split:
        draws = jax.random.uniform(jax.random.fold_in(jax.random.fold_in(stream_key, 6), position), (parts,), jnp.float32, least / len(split), largest / len(split))
        gain = gain * jnp.repeat(jnp.exp(draws), dims[position] // parts).reshape((-1,) + (1,) * (len(dims) - 1 - position))
    return gain


def cumulative_ranks(number_of, skew):
    portions = [(1 << 20) // math.isqrt(standing ** skew) + 1 for standing in range(1, number_of + 1)]
    width = 1 + sum(portions) // (1 << 30)
    return np.cumsum(np.array([max(1, weight // width) for weight in portions]))


def ranked(key, extent, count, skew):
    table = cumulative_ranks(count, skew)
    pick = jax.random.randint(jax.random.fold_in(key, 1), extent, 0, int(table[count - 1]))
    rank = jnp.searchsorted(jnp.asarray(table, jnp.int32), pick, side="right")
    return jax.random.permutation(jax.random.fold_in(key, 2), count)[rank].astype(jnp.int32)


def centred(key, extent, deviation, limit, shards=(), held_as=jnp.bfloat16):
    loudness = block_scale(key, extent, shards, -0.22, 0.18) if shards else 1.0
    result = jax.random.normal(key, extent, jnp.float32) * deviation * loudness
    return jnp.minimum(jnp.maximum(result, -limit), limit).astype(held_as)


def setup_inputs(seed: int = 0) -> dict:
    key_list = jax.random.split(jax.random.key(seed), 9)
    return {
        "feature_ids": touch_ends(ranked(key_list[0], (FEATS, BATCH, HOTS), VOCAB, 2), jax.random.fold_in(key_list[0], 3), 0, VOCAB - 1).astype(jnp.int32),
        "tables": centred(key_list[1], (FEATS, VOCAB, EMBED), 0.35, 5.0, ((0, 8),)),
        "table_of_feature": jax.random.permutation(key_list[2], FEATS).astype(jnp.int32),
        "cross_down": centred(key_list[3], (LAYERS, WIDTH, RANK), WIDTH ** -0.5, 0.1875, ((1, 4),)),
        "cross_up": centred(key_list[4], (LAYERS, WIDTH, RANK), (4 * RANK) ** -0.5, 0.125, ((1, 4),)),
        "cross_bias": centred(key_list[5], (LAYERS, WIDTH), 0.5, 3.0, ((1, 4),), jnp.float32),
        "tower_weight": centred(key_list[6], (WIDTH, HID), WIDTH ** -0.5, 0.1875, ((0, 8), (1, 4))),
        "tower_bias": centred(key_list[7], (HID,), 0.5, 3.0, ((0, 4),), jnp.float32),
    }


def pool_table(pair):
    table, id_rows = pair
    summed = jnp.zeros((id_rows.shape[0], table.shape[1]), jnp.float32)
    for hot_index in range(HOTS):
        summed = summed + jnp.take(table, id_rows[:, hot_index], axis=0).astype(jnp.float32)
    return summed.astype(jnp.bfloat16)


def reference(feature_ids, tables, table_of_feature, cross_down, cross_up, cross_bias, tower_weight, tower_bias):
    pooled = lax.map(pool_table, (tables, feature_ids))
    ordered = jnp.take(pooled, table_of_feature, axis=0)
    embedded = jnp.transpose(ordered, (1, 0, 2)).reshape(BATCH, WIDTH)
    embedded_wide = embedded.astype(jnp.float32)
    crossed = embedded
    for layer_index in range(LAYERS):
        projected = jnp.dot(crossed, cross_down[layer_index], preferred_element_type=jnp.float32).astype(jnp.bfloat16)
        lifted = lax.dot_general(projected, cross_up[layer_index], (((1,), (1,)), ((), ())), preferred_element_type=jnp.float32)
        crossed = (embedded_wide * (lifted + cross_bias[layer_index]) + crossed.astype(jnp.float32)).astype(jnp.bfloat16)
    pre_act = jnp.dot(crossed, tower_weight, preferred_element_type=jnp.float32) + tower_bias
    return jax.nn.relu(pre_act).astype(jnp.bfloat16)
```

```python
import functools

import jax
import jax.numpy as jnp
from jax import lax
from jax.experimental import pallas as pl
from jax.experimental.pallas import tpu as pltpu
from jax.sharding import PartitionSpec as P


GATHER_LIMIT = 12 * 2**20

VMEM = pl.BlockSpec(memory_space=pltpu.VMEM)
SMEM = pl.BlockSpec(memory_space=pltpu.SMEM)


def reduce_body(
    feature_ids,
    tables,
    table_of_feature,
    cross_down,
    cross_up,
    cross_bias,
    tower_weight,
    tower_bias,
):
    groups = lax.axis_size("dp")
    members = lax.axis_size("mp")
    member = lax.axis_index("mp")
    table_count, batch_size, hot_count = feature_ids.shape
    row_count = batch_size // (groups * members)
    shaped = feature_ids[0].reshape(groups, members, row_count, hot_count)
    own_ids = lax.dynamic_index_in_dim(shaped, member, 1, keepdims=False).reshape(
        groups * row_count, hot_count
    )
    summed = jnp.zeros((groups * row_count, tables.shape[2]), jnp.float32)
    for hot_index in range(hot_count):
        summed = summed + jnp.take(tables[0], own_ids[:, hot_index], axis=0).astype(jnp.float32)
    columns = [summed.astype(jnp.bfloat16)]
    pooled = jnp.stack(columns, axis=1)
    regrouped = lax.all_to_all(pooled, "dp", split_axis=0, concat_axis=1, tiled=True)
    ordered = jnp.take(regrouped, table_of_feature, axis=1)
    by_width = lax.all_to_all(ordered, "mp", split_axis=1, concat_axis=0, tiled=True)
    group_rows = by_width.shape[0]
    embedded = by_width.reshape(group_rows, -1)
    embedded_wide = embedded.astype(jnp.float32)
    crossed = embedded
    layer_total = cross_down.shape[0]
    for layer_index in range(layer_total):
        partial_value = jnp.dot(
            crossed, cross_down[layer_index], preferred_element_type=jnp.float32
        )
        projected = lax.psum(partial_value.astype(jnp.bfloat16), "mp")
        lifted = lax.dot_general(
            projected,
            cross_up[layer_index],
            (((1,), (1,)), ((), ())),
            preferred_element_type=jnp.float32,
        )
        crossed = (
            embedded_wide * (lifted + cross_bias[layer_index]) + crossed.astype(jnp.float32)
        ).astype(jnp.bfloat16)
    full_rows = lax.all_gather(crossed, "mp", axis=1, tiled=True)
    pre_act = jnp.dot(
        full_rows,
        lax.all_gather(tower_weight, "dp", axis=0, tiled=True),
        preferred_element_type=jnp.float32,
    )
    return jax.nn.relu(pre_act + tower_bias).astype(jnp.bfloat16)


def pool_kernel(chunk, place_ref, ids_ref, table_ref, keep_ref, send_ref):
    vocab, embed = table_ref.shape
    hots, samples = ids_ref.shape
    groups = 2 * keep_ref.shape[0]
    rows = samples // groups
    ids = ids_ref[...]
    total = jnp.zeros((embed, samples), jnp.float32)
    row_at = lax.broadcasted_iota(jnp.int16, (chunk, samples), 0)
    one = jnp.ones((), jnp.bfloat16)
    zero = jnp.zeros((), jnp.bfloat16)
    for start in range(0, vocab, chunk):
        shifted = (ids - start).astype(jnp.int16)
        counts = None
        for hot in range(hots):
            term = jnp.where(shifted[hot : hot + 1, :] == row_at, one, zero)
            counts = term if counts is None else counts + term
        total = total + lax.dot_general(
            table_ref[start : start + chunk, :],
            counts,
            (((0,), (0,)), ((), ())),
            preferred_element_type=jnp.float32,
        )
    pooled = total.T.astype(jnp.bfloat16)
    group = place_ref[0]
    core = lax.rem(group, 2)
    half = lax.div(group, 2)
    for chip in range(groups // 2):
        at = jnp.bitwise_xor(half, chip)
        low = pooled[2 * chip * rows : (2 * chip + 1) * rows]
        high = pooled[(2 * chip + 1) * rows : (2 * chip + 2) * rows]
        keep_ref[at] = jnp.where(core == 0, low, high)
        send_ref[at] = jnp.where(core == 0, high, low)


def fill_layer(layer, place_ref, down_ref, up_ref, own_ref, other_ref, down_full, up_full):
    members = own_ref.shape[1] + 1
    chips = own_ref.shape[0]
    block, rank = down_ref.shape[1:]
    rows = own_ref.shape[3]
    group, member = place_ref[0], place_ref[1]
    base = pl.multiple_of(member * block, block)
    down_full[pl.ds(base, block), :] = down_ref[layer]
    up_full[pl.ds(base, block), :] = up_ref[layer]
    for step in range(1, members):
        owner = lax.rem(member + members - step, members)
        for chip in range(chips):
            for core, source in enumerate((own_ref, other_ref)):
                slot = jnp.bitwise_xor(group, 2 * chip + core)
                at = pl.multiple_of(owner * block + slot * rows, rows)
                down_full[pl.ds(at, rows), :] = source[chip, step - 1, 0]
                up_full[pl.ds(at, rows), :] = source[chip, step - 1, 1]


def cross_step(layer, embedded, crossed, down_full, up_full, bias):
    projected = jnp.dot(
        crossed, down_full[...], preferred_element_type=jnp.float32
    ).astype(jnp.bfloat16)
    lifted = lax.dot_general(
        projected, up_full[...], (((1,), (1,)), ((), ())), preferred_element_type=jnp.float32
    )
    return (
        embedded.astype(jnp.float32) * (lifted + bias[layer : layer + 1, :])
        + crossed.astype(jnp.float32)
    ).astype(jnp.bfloat16)


def first_kernel(members, *refs):
    place_ref, order_ref, down_ref, up_ref, own_ref, other_ref = refs[:6]
    bias_refs = refs[6 : 6 + members]
    piece_refs = refs[6 + members : 6 + 2 * members]
    embedded_ref, crossed_ref, bias_ref, down_full, up_full = refs[6 + 2 * members :]
    group, member = place_ref[0], place_ref[1]
    tables, rows, embed = piece_refs[0].shape
    block = down_ref.shape[1]
    for feature in range(tables):
        slot = jnp.bitwise_xor(order_ref[feature], group)
        for step in range(members):
            embedded_ref[
                step * rows : (step + 1) * rows, feature * embed : (feature + 1) * embed
            ] = piece_refs[step][slot]
    for step in range(members):
        owner = lax.rem(member + members - step, members)
        bias_ref[:, pl.ds(pl.multiple_of(owner * block, block), block)] = bias_refs[step][...]
    fill_layer(0, place_ref, down_ref, up_ref, own_ref, other_ref, down_full, up_full)
    embedded = embedded_ref[...]
    crossed_ref[...] = cross_step(0, embedded, embedded, down_full, up_full, bias_ref)


def last_kernel(
    members,
    place_ref,
    down_ref,
    up_ref,
    own_ref,
    other_ref,
    tower_own_ref,
    tower_other_ref,
    tower_bias_ref,
    embedded_ref,
    crossed_ref,
    bias_ref,
    hidden_ref,
    down_full,
    up_full,
    tower_full,
):
    group, member = place_ref[0], place_ref[1]
    layers = down_ref.shape[0]
    for layer in range(1, layers):
        fill_layer(
            layer,
            place_ref,
            down_ref,
            up_ref,
            own_ref.at[layer - 1],
            other_ref.at[layer - 1],
            down_full.at[layer - 1],
            up_full.at[layer - 1],
        )
    chips, depth, _ = tower_own_ref.shape
    for chip in range(chips):
        for core, source in enumerate((tower_own_ref, tower_other_ref)):
            slot = jnp.bitwise_xor(group, 2 * chip + core)
            tower_full[pl.ds(pl.multiple_of(slot * depth, depth), depth), :] = source[chip]
    embedded = embedded_ref[...]
    crossed = crossed_ref[...]
    for layer in range(1, layers):
        crossed = cross_step(
            layer, embedded, crossed, down_full.at[layer - 1], up_full.at[layer - 1], bias_ref
        )
    pre_act = jnp.dot(crossed, tower_full[...], preferred_element_type=jnp.float32)
    hidden = jnp.maximum(pre_act + tower_bias_ref[...], 0.0).astype(jnp.bfloat16)
    rows = hidden.shape[0] // members
    for step in range(members):
        owner = lax.rem(member + members - step, members)
        hidden_ref[pl.ds(pl.multiple_of(owner * rows, rows), rows), :] = hidden[
            step * rows : (step + 1) * rows
        ]


def shift_over(value, axis, step):
    count = lax.axis_size(axis)
    return lax.ppermute(value, axis, [(i, (i + step) % count) for i in range(count)])


def flip_over(value, axis, mask):
    count = lax.axis_size(axis)
    return lax.ppermute(value, axis, [(i, i ^ mask) for i in range(count)])


def gather_body(
    feature_ids,
    tables,
    table_of_feature,
    cross_down,
    cross_up,
    cross_bias,
    tower_weight,
    tower_bias,
):
    groups = lax.axis_size("dp")
    members = lax.axis_size("mp")
    group = lax.axis_index("dp")
    member = lax.axis_index("mp")
    place = jnp.stack([group, member]).astype(jnp.int32)
    _, batch, hots = feature_ids.shape
    rows = batch // (groups * members)
    _, vocab, embed = tables.shape
    layers, block, rank = cross_down.shape
    width = block * members
    slice_rows = block // groups
    chips = groups // 2

    down_slice = lax.dynamic_slice_in_dim(cross_down, group * slice_rows, slice_rows, 1)
    up_slice = lax.dynamic_slice_in_dim(cross_up, group * slice_rows, slice_rows, 1)
    legs = []
    for layer in range(layers):
        payload = jnp.stack([down_slice[layer], up_slice[layer]])
        legs.append([shift_over(payload, "mp", step) for step in range(1, members)])
    biases = [cross_bias] + [shift_over(cross_bias, "mp", step) for step in range(1, members)]

    tower_own = jnp.stack(
        [tower_weight] + [flip_over(tower_weight, "dp", 2 * chip) for chip in range(1, chips)]
    )
    tower_other = flip_over(tower_own, "dp", 1)

    ids = feature_ids[0].T.reshape(hots, groups, members, rows)
    own_ids = lax.dynamic_index_in_dim(ids, member, 2, keepdims=False).reshape(
        hots, groups * rows
    )
    keep, send = pl.pallas_call(
        functools.partial(pool_kernel, 256),
        out_shape=[jax.ShapeDtypeStruct((chips, rows, embed), jnp.bfloat16)] * 2,
        in_specs=[SMEM, VMEM, VMEM],
        out_specs=[VMEM, VMEM],
        cost_estimate=pl.CostEstimate(
            flops=4 * vocab * groups * rows * embed, bytes_accessed=2**21, transcendentals=0
        ),
        name="pool",
    )(place, own_ids, tables[0])
    crossing = flip_over(send, "dp", 1)
    both = jnp.stack([keep, crossing], axis=1)
    held = [both[0]] + [flip_over(both[chip], "dp", 2 * chip) for chip in range(1, chips)]
    piece = jnp.concatenate(held)
    pieces = [piece] + [shift_over(piece, "mp", step) for step in range(1, members)]

    owns, others = [], []
    for layer in range(layers):
        got = jnp.stack(legs[layer])
        own = jnp.stack([got] + [flip_over(got, "dp", 2 * chip) for chip in range(1, chips)])
        owns.append(own)
        others.append(flip_over(own, "dp", 1))

    samples = rows * members
    embedded, crossed, bias = pl.pallas_call(
        functools.partial(first_kernel, members),
        out_shape=[
            jax.ShapeDtypeStruct((samples, width), jnp.bfloat16),
            jax.ShapeDtypeStruct((samples, width), jnp.bfloat16),
            jax.ShapeDtypeStruct((layers, width), jnp.float32),
        ],
        in_specs=[SMEM, SMEM] + [VMEM] * (4 + 2 * members),
        out_specs=[VMEM] * 3,
        scratch_shapes=[pltpu.VMEM((width, rank), jnp.bfloat16)] * 2,
        cost_estimate=pl.CostEstimate(
            flops=4 * samples * width * rank, bytes_accessed=2**22, transcendentals=0
        ),
        name="cross_first",
    )(place, table_of_feature, cross_down, cross_up, owns[0], others[0], *biases, *pieces)
    units = tower_weight.shape[1]
    return pl.pallas_call(
        functools.partial(last_kernel, members),
        out_shape=jax.ShapeDtypeStruct((samples, units), jnp.bfloat16),
        in_specs=[SMEM] + [VMEM] * 10,
        out_specs=VMEM,
        scratch_shapes=[pltpu.VMEM((layers - 1, width, rank), jnp.bfloat16)] * 2
        + [pltpu.VMEM((width, units), jnp.bfloat16)],
        cost_estimate=pl.CostEstimate(
            flops=8 * samples * width * rank, bytes_accessed=2**22, transcendentals=0
        ),
        name="cross_last",
    )(
        place,
        cross_down,
        cross_up,
        jnp.stack(owns[1:]),
        jnp.stack(others[1:]),
        tower_own,
        tower_other,
        tower_bias.reshape(1, units),
        embedded,
        crossed,
        bias,
    )


def solution(mesh):
    def body(*args):
        cross_down = args[3]
        gathered = 2 * 2 * cross_down.size * lax.axis_size("mp")
        plan = gather_body if gathered <= GATHER_LIMIT else reduce_body
        return plan(*args)

    return jax.shard_map(
        body,
        mesh=mesh,
        in_specs=(
            P("dp", None, None),
            P("dp", None, None),
            P(),
            P(None, "mp", None),
            P(None, "mp", None),
            P(None, "mp"),
            P("dp", "mp"),
            P("mp"),
        ),
        out_specs=P("dp", "mp"),
        check_vma=False,
    )
```

```python
import functools

import jax
import jax.numpy as jnp
from jax import lax
from jax.experimental import pallas as pl
from jax.experimental.pallas import tpu as pltpu
from jax.sharding import PartitionSpec as P


GATHER_LIMIT = 12 * 2**20

LANES = 128
SUBLANES = 16

VMEM = pl.BlockSpec(memory_space=pltpu.VMEM)
SMEM = pl.BlockSpec(memory_space=pltpu.SMEM)


def reduce_body(
    feature_ids,
    tables,
    table_of_feature,
    cross_down,
    cross_up,
    cross_bias,
    tower_weight,
    tower_bias,
):
    groups = lax.axis_size("dp")
    members = lax.axis_size("mp")
    member = lax.axis_index("mp")
    _, batch_size, hot_count = feature_ids.shape
    row_count = batch_size // (groups * members)
    shaped = feature_ids[0].reshape(groups, members, row_count, hot_count)
    own_ids = lax.dynamic_index_in_dim(shaped, member, 1, keepdims=False).reshape(
        groups * row_count, hot_count
    )
    summed = jnp.zeros((groups * row_count, tables.shape[2]), jnp.float32)
    for hot_index in range(hot_count):
        summed = summed + jnp.take(tables[0], own_ids[:, hot_index], axis=0).astype(jnp.float32)
    columns = [summed.astype(jnp.bfloat16)]
    pooled = jnp.stack(columns, axis=1)
    regrouped = lax.all_to_all(pooled, "dp", split_axis=0, concat_axis=1, tiled=True)
    ordered = jnp.take(regrouped, table_of_feature, axis=1)
    by_width = lax.all_to_all(ordered, "mp", split_axis=1, concat_axis=0, tiled=True)
    group_rows = by_width.shape[0]
    embedded = by_width.reshape(group_rows, -1)
    embedded_wide = embedded.astype(jnp.float32)
    crossed = embedded
    layer_total = cross_down.shape[0]
    for layer_index in range(layer_total):
        partial_value = jnp.dot(
            crossed, cross_down[layer_index], preferred_element_type=jnp.float32
        )
        projected = lax.psum(partial_value.astype(jnp.bfloat16), "mp")
        lifted = lax.dot_general(
            projected,
            cross_up[layer_index],
            (((1,), (1,)), ((), ())),
            preferred_element_type=jnp.float32,
        )
        crossed = (
            embedded_wide * (lifted + cross_bias[layer_index]) + crossed.astype(jnp.float32)
        ).astype(jnp.bfloat16)
    full_rows = lax.all_gather(crossed, "mp", axis=1, tiled=True)
    pre_act = jnp.dot(
        full_rows,
        lax.all_gather(tower_weight, "dp", axis=0, tiled=True),
        preferred_element_type=jnp.float32,
    )
    return jax.nn.relu(pre_act + tower_bias).astype(jnp.bfloat16)


def params(mib):
    return pltpu.CompilerParams(vmem_limit_bytes=mib * 2**20)


def pool_kernel(chunk, place_ref, ids_ref, source_ref, keep_ref, send_ref, table_ref, arrived):
    vocab, embed = table_ref.shape
    pieces = arrived.shape[0]
    size = vocab // pieces
    copies = [
        pltpu.make_async_copy(
            source_ref.at[pl.ds(index * size, size)],
            table_ref.at[pl.ds(index * size, size)],
            arrived.at[index],
        )
        for index in range(pieces)
    ]
    for copy in copies:
        copy.start()
    hots, batch = ids_ref.shape
    chips, rows, _ = keep_ref.shape
    groups = 2 * chips
    samples = groups * rows
    per_group = batch // groups
    group, member = place_ref[0], place_ref[1]
    parts = []
    for owner in range(groups):
        if rows == LANES // 2:
            at = pl.multiple_of(owner * per_group + lax.div(member, 2) * LANES, LANES)
            wide = ids_ref[:, pl.ds(at, LANES)]
            parts.append(jnp.where(lax.rem(member, 2) == 0, wide[:, :rows], wide[:, rows:]))
        else:
            at = pl.multiple_of(owner * per_group + member * rows, LANES)
            parts.append(ids_ref[:, pl.ds(at, rows)])
    ids = jnp.concatenate(parts, axis=1)
    total = jnp.zeros((embed, samples), jnp.float32)
    row_at = lax.broadcasted_iota(jnp.int16, (chunk, samples), 0)
    one = jnp.ones((), jnp.bfloat16)
    zero = jnp.zeros((), jnp.bfloat16)
    for start in range(0, vocab, chunk):
        shifted = (ids - start).astype(jnp.int16)
        counts = None
        for hot in range(hots):
            term = jnp.where(shifted[hot : hot + 1, :] == row_at, one, zero)
            counts = term if counts is None else counts + term
        if start % size == 0:
            copies[start // size].wait()
        total = total + lax.dot_general(
            table_ref[start : start + chunk, :],
            counts,
            (((0,), (0,)), ((), ())),
            preferred_element_type=jnp.float32,
        )
    pooled = total.T.astype(jnp.bfloat16)
    core = lax.rem(group, 2)
    half = lax.div(group, 2)
    for chip in range(chips):
        at = jnp.bitwise_xor(half, chip)
        low = pooled[2 * chip * rows : (2 * chip + 1) * rows]
        high = pooled[(2 * chip + 1) * rows : (2 * chip + 2) * rows]
        keep_ref[at] = jnp.where(core == 0, low, high)
        send_ref[at] = jnp.where(core == 0, high, low)


def cross_kernel(members, chips, *refs):
    refs = list(refs)

    def take(count):
        taken = refs[:count]
        del refs[:count]
        return taken

    place_ref, order_ref, down_ref, up_ref, bias_ref, tower_bias_ref = take(6)
    own_refs, other_refs = take(chips), take(chips)
    tower_own_refs, tower_other_refs = take(chips), take(chips)
    piece_refs = take(members)
    (hidden_ref,) = take(1)
    embedded_ref, bias_full, down_full, up_full, tower_full = take(5)

    group, member = place_ref[0], place_ref[1]
    layers, block, _ = down_ref.shape
    tables = order_ref.shape[0]
    rows = hidden_ref.shape[0] // members
    embed = piece_refs[0].shape[1]
    slice_rows = block // (2 * chips)

    for feature in range(tables):
        slot = jnp.bitwise_xor(order_ref[feature], group)
        for step in range(members):
            embedded_ref[
                step * rows : (step + 1) * rows, feature * embed : (feature + 1) * embed
            ] = piece_refs[step][pl.ds(pl.multiple_of(slot * rows, rows), rows), :]

    base = pl.multiple_of(member * block, block)
    bias_full[:, pl.ds(base, block)] = bias_ref[...]
    for step in range(1, members):
        owner = lax.rem(member + members - step, members)
        for layer in range(layers):
            for part in range(block // embed):
                at = tables * rows + (layer * block) // embed + part
                count = layers * block // embed
                bias = sum(
                    piece_refs[step][at + term * count, :].astype(jnp.float32).reshape(1, embed)
                    for term in range(3)
                )
                lane = pl.multiple_of(owner * block + part * embed, embed)
                bias_full[layer : layer + 1, pl.ds(lane, embed)] = bias

    for chip in range(chips):
        for core, source in enumerate((tower_own_refs[chip], tower_other_refs[chip])):
            depth = source.shape[0]
            slot = jnp.bitwise_xor(group, 2 * chip + core)
            tower_full[pl.ds(pl.multiple_of(slot * depth, depth), depth), :] = source[...]

    for layer in range(layers):
        down_full[layer, pl.ds(base, block), :] = down_ref[layer]
        up_full[layer, pl.ds(base, block), :] = up_ref[layer]
        first = 2 * layer * slice_rows
        for step in range(1, members):
            owner = lax.rem(member + members - step, members)
            for chip in range(chips):
                for core, source in enumerate((own_refs[chip], other_refs[chip])):
                    slot = jnp.bitwise_xor(group, 2 * chip + core)
                    at = pl.multiple_of(owner * block + slot * slice_rows, slice_rows)
                    down_full[layer, pl.ds(at, slice_rows), :] = source[
                        step - 1, first : first + slice_rows
                    ]
                    up_full[layer, pl.ds(at, slice_rows), :] = source[
                        step - 1, first + slice_rows : first + 2 * slice_rows
                    ]

    embedded = embedded_ref[...]
    crossed = embedded
    for layer in range(layers):
        projected = jnp.dot(
            crossed, down_full[layer], preferred_element_type=jnp.float32
        ).astype(jnp.bfloat16)
        lifted = lax.dot_general(
            projected,
            up_full[layer],
            (((1,), (1,)), ((), ())),
            preferred_element_type=jnp.float32,
        )
        crossed = (
            embedded.astype(jnp.float32) * (lifted + bias_full[layer : layer + 1, :])
            + crossed.astype(jnp.float32)
        ).astype(jnp.bfloat16)

    pre_act = jnp.dot(crossed, tower_full[...], preferred_element_type=jnp.float32)
    hidden = jnp.maximum(pre_act + tower_bias_ref[...], 0.0).astype(jnp.bfloat16)
    for step in range(members):
        owner = lax.rem(member + members - step, members)
        hidden_ref[pl.ds(pl.multiple_of(owner * rows, rows), rows), :] = hidden[
            step * rows : (step + 1) * rows
        ]


def shift_over(value, axis, step):
    count = lax.axis_size(axis)
    return lax.ppermute(value, axis, [(i, (i + step) % count) for i in range(count)])


def flip_over(value, axis, mask):
    count = lax.axis_size(axis)
    return lax.ppermute(value, axis, [(i, i ^ mask) for i in range(count)])


def split_three(value):
    high = lax.reduce_precision(value, 8, 7)
    rest = value - high
    middle = lax.reduce_precision(rest, 8, 7)
    return [term.astype(jnp.bfloat16) for term in (high, middle, rest - middle)]


def gather_body(
    feature_ids,
    tables,
    table_of_feature,
    cross_down,
    cross_up,
    cross_bias,
    tower_weight,
    tower_bias,
):
    groups = lax.axis_size("dp")
    members = lax.axis_size("mp")
    group = lax.axis_index("dp")
    member = lax.axis_index("mp")
    place = jnp.stack([group, member]).astype(jnp.int32)
    _, batch, _ = feature_ids.shape
    rows = batch // (groups * members)
    _, vocab, embed = tables.shape
    layers, block, rank = cross_down.shape
    width = block * members
    slice_rows = block // groups
    chips = groups // 2
    steps = range(1, members)

    down_slice = lax.dynamic_slice_in_dim(cross_down, group * slice_rows, slice_rows, 1)
    up_slice = lax.dynamic_slice_in_dim(cross_up, group * slice_rows, slice_rows, 1)
    matrices = []
    for layer in range(layers):
        matrices += [down_slice[layer], up_slice[layer]]
    payload = jnp.concatenate(matrices)
    legs = [shift_over(payload, "mp", step) for step in steps]

    keep, send = pl.pallas_call(
        functools.partial(pool_kernel, 256),
        out_shape=[jax.ShapeDtypeStruct((chips, rows, embed), jnp.bfloat16)] * 2,
        in_specs=[SMEM, VMEM, pl.BlockSpec(memory_space=pl.ANY)],
        out_specs=[VMEM, VMEM],
        scratch_shapes=[pltpu.VMEM((vocab, embed), jnp.bfloat16), pltpu.SemaphoreType.DMA((4,))],
        compiler_params=params(16),
        cost_estimate=pl.CostEstimate(
            flops=4 * vocab * groups * rows * embed, bytes_accessed=2**21, transcendentals=0
        ),
        name="pool",
    )(place, feature_ids[0].T, tables[0])
    crossing = flip_over(send, "dp", 1)
    both = jnp.stack([keep, crossing], axis=1)
    held = [both[0]] + [flip_over(both[chip], "dp", 2 * chip) for chip in range(1, chips)]
    terms = jnp.stack(split_three(cross_bias.reshape(-1))).reshape(-1, embed)
    bias_rows = -(-terms.shape[0] // SUBLANES) * SUBLANES
    terms = jnp.pad(terms, ((0, bias_rows - terms.shape[0]), (0, 0)))
    piece = jnp.concatenate([part.reshape(-1, embed) for part in held] + [terms])

    got = jnp.stack([leg for leg in legs])
    own = [got] + [flip_over(got, "dp", 2 * chip) for chip in range(1, chips)]
    other = [flip_over(own[chip], "dp", 1) for chip in range(chips)]
    pieces = [piece] + [shift_over(piece, "mp", step) for step in steps]

    tower_own = [tower_weight] + [
        flip_over(tower_weight, "dp", 2 * chip) for chip in range(1, chips)
    ]
    tower_other = [flip_over(tower_own[chip], "dp", 1) for chip in range(chips)]

    samples = rows * members
    units = tower_weight.shape[1]
    inputs = [place, table_of_feature, cross_down, cross_up, cross_bias]
    inputs += [tower_bias.reshape(1, units)]
    inputs += own + other + tower_own + tower_other + pieces
    return pl.pallas_call(
        functools.partial(cross_kernel, members, chips),
        out_shape=jax.ShapeDtypeStruct((samples, units), jnp.bfloat16),
        in_specs=[SMEM, SMEM] + [VMEM] * (len(inputs) - 2),
        out_specs=VMEM,
        scratch_shapes=[
            pltpu.VMEM((samples, width), jnp.bfloat16),
            pltpu.VMEM((layers, width), jnp.float32),
            pltpu.VMEM((layers, width, rank), jnp.bfloat16),
            pltpu.VMEM((layers, width, rank), jnp.bfloat16),
            pltpu.VMEM((width, units), jnp.bfloat16),
        ],
        compiler_params=params(32),
        cost_estimate=pl.CostEstimate(
            flops=2 * samples * width * (2 * layers * rank + units),
            bytes_accessed=2**23,
            transcendentals=0,
        ),
        name="cross",
    )(*inputs)


def solution(mesh):
    groups, members = mesh.shape["dp"], mesh.shape["mp"]

    def body(*args):
        feature_ids, tables, cross_down = args[0], args[1], args[3]
        _, block, _ = cross_down.shape
        rows = feature_ids.shape[1] // (groups * members)
        fits = 4 * cross_down.size * members <= GATHER_LIMIT
        fits = fits and block % tables.shape[2] == 0 and block % (SUBLANES * groups) == 0
        fits = fits and (rows == LANES // 2 or rows % LANES == 0) and groups & (groups - 1) == 0
        return (gather_body if fits else reduce_body)(*args)

    return jax.shard_map(
        body,
        mesh=mesh,
        in_specs=(
            P("dp", None, None),
            P("dp", None, None),
            P(),
            P(None, "mp", None),
            P(None, "mp", None),
            P(None, "mp"),
            P("dp", "mp"),
            P("mp"),
        ),
        out_specs=P("dp", "mp"),
        check_vma=False,
    )
```

```python
import functools

import jax
import jax.numpy as jnp
from jax import lax
from jax.experimental import pallas as pl
from jax.experimental.pallas import tpu as pltpu
from jax.sharding import PartitionSpec as P


GATHER_LIMIT = 12 * 2**20

LANES = 128
SUBLANES = 16
PLANE = 4

VMEM = pl.BlockSpec(memory_space=pltpu.VMEM)
SMEM = pl.BlockSpec(memory_space=pltpu.SMEM)


def reduce_body(
    feature_ids,
    tables,
    table_of_feature,
    cross_down,
    cross_up,
    cross_bias,
    tower_weight,
    tower_bias,
):
    groups = lax.axis_size("dp")
    members = lax.axis_size("mp")
    member = lax.axis_index("mp")
    _, batch_size, hot_count = feature_ids.shape
    row_count = batch_size // (groups * members)
    shaped = feature_ids[0].reshape(groups, members, row_count, hot_count)
    own_ids = lax.dynamic_index_in_dim(shaped, member, 1, keepdims=False).reshape(
        groups * row_count, hot_count
    )
    summed = jnp.zeros((groups * row_count, tables.shape[2]), jnp.float32)
    for hot_index in range(hot_count):
        summed = summed + jnp.take(tables[0], own_ids[:, hot_index], axis=0).astype(jnp.float32)
    columns = [summed.astype(jnp.bfloat16)]
    pooled = jnp.stack(columns, axis=1)
    regrouped = lax.all_to_all(pooled, "dp", split_axis=0, concat_axis=1, tiled=True)
    ordered = jnp.take(regrouped, table_of_feature, axis=1)
    by_width = lax.all_to_all(ordered, "mp", split_axis=1, concat_axis=0, tiled=True)
    group_rows = by_width.shape[0]
    embedded = by_width.reshape(group_rows, -1)
    embedded_wide = embedded.astype(jnp.float32)
    crossed = embedded
    layer_total = cross_down.shape[0]
    for layer_index in range(layer_total):
        partial_value = jnp.dot(
            crossed, cross_down[layer_index], preferred_element_type=jnp.float32
        )
        projected = lax.psum(partial_value.astype(jnp.bfloat16), "mp")
        lifted = lax.dot_general(
            projected,
            cross_up[layer_index],
            (((1,), (1,)), ((), ())),
            preferred_element_type=jnp.float32,
        )
        crossed = (
            embedded_wide * (lifted + cross_bias[layer_index]) + crossed.astype(jnp.float32)
        ).astype(jnp.bfloat16)
    full_rows = lax.all_gather(crossed, "mp", axis=1, tiled=True)
    pre_act = jnp.dot(
        full_rows,
        lax.all_gather(tower_weight, "dp", axis=0, tiled=True),
        preferred_element_type=jnp.float32,
    )
    return jax.nn.relu(pre_act + tower_bias).astype(jnp.bfloat16)


def params(mib):
    return pltpu.CompilerParams(vmem_limit_bytes=mib * 2**20)


def pool_kernel(
    chunk, ids_ref, bias_ref, table_ref, keep_ref, send_ref, terms_ref
):
    vocab, embed = table_ref.shape
    rest = bias_ref[...]
    layers, block = rest.shape
    parts = block // embed
    terms_ref[...] = jnp.zeros_like(terms_ref)
    for term in range(3):
        rounded = rest.astype(jnp.bfloat16)
        for layer in range(layers):
            for part in range(parts):
                terms_ref[pl.ds((term * layers + layer) * parts + part, 1), :] = rounded[
                    layer : layer + 1, part * embed : (part + 1) * embed
                ]
        rest = rest - rounded.astype(jnp.float32)
    hots, batch = ids_ref.shape
    chips, rows, _ = keep_ref.shape
    groups = 2 * chips
    samples = groups * rows
    per_group = batch // groups
    group, member = lax.axis_index("dp"), lax.axis_index("mp")
    wanted = []
    for owner in range(groups):
        if rows == LANES // 2:
            at = pl.multiple_of(owner * per_group + lax.div(member, 2) * LANES, LANES)
            wide = ids_ref[:, pl.ds(at, LANES)]
            wanted.append(jnp.where(lax.rem(member, 2) == 0, wide[:, :rows], wide[:, rows:]))
        else:
            at = pl.multiple_of(owner * per_group + member * rows, LANES)
            wanted.append(ids_ref[:, pl.ds(at, rows)])
    ids = jnp.concatenate(wanted, axis=1)
    total = jnp.zeros((embed, samples), jnp.float32)
    row_at = lax.broadcasted_iota(jnp.int16, (chunk, samples), 0)
    one = jnp.ones((), jnp.bfloat16)
    zero = jnp.zeros((), jnp.bfloat16)
    for start in range(0, vocab, chunk):
        shifted = (ids - start).astype(jnp.int16)
        counts = None
        for hot in range(hots):
            term = jnp.where(shifted[hot : hot + 1, :] == row_at, one, zero)
            counts = term if counts is None else counts + term
        total = total + lax.dot_general(
            table_ref[start : start + chunk, :],
            counts,
            (((0,), (0,)), ((), ())),
            preferred_element_type=jnp.float32,
        )
    pooled = total.T.astype(jnp.bfloat16)
    core = lax.rem(group, 2)
    half = lax.div(group, 2)
    for chip in range(chips):
        at = jnp.bitwise_xor(half, chip)
        low = pooled[2 * chip * rows : (2 * chip + 1) * rows]
        high = pooled[(2 * chip + 1) * rows : (2 * chip + 2) * rows]
        keep_ref[at] = jnp.where(core == 0, low, high)
        send_ref[at] = jnp.where(core == 0, high, low)


def cross_kernel(members, chips, *refs):
    refs = list(refs)

    def take(count):
        taken = refs[:count]
        del refs[:count]
        return taken

    order_ref, down_ref, up_ref, tower_bias_ref = take(4)
    own_refs, other_refs = take(chips), take(chips)
    tower_own_refs, tower_other_refs = take(chips), take(chips)
    piece_refs = take(members)
    (hidden_ref,) = take(1)
    embedded_ref, bias_full, down_full, up_full, tower_full = take(5)

    group, member = lax.axis_index("dp"), lax.axis_index("mp")
    layers, block, _ = down_ref.shape
    tables = order_ref.shape[0]
    rows = hidden_ref.shape[0] // members
    embed = piece_refs[0].shape[1]
    slice_rows = block // (2 * chips)

    for feature in range(tables):
        slot = jnp.bitwise_xor(order_ref[feature], group)
        for step in range(members):
            embedded_ref[
                step * rows : (step + 1) * rows, feature * embed : (feature + 1) * embed
            ] = piece_refs[step][pl.ds(pl.multiple_of(slot * rows, rows), rows), :]

    base = pl.multiple_of(member * block, block)
    for step in range(members):
        owner = jnp.bitwise_xor(member, step)
        for layer in range(layers):
            for part in range(block // embed):
                at = tables * rows + (layer * block) // embed + part
                count = layers * block // embed
                bias = sum(
                    piece_refs[step][at + term * count, :].astype(jnp.float32).reshape(1, embed)
                    for term in range(3)
                )
                lane = pl.multiple_of(owner * block + part * embed, embed)
                bias_full[layer : layer + 1, pl.ds(lane, embed)] = bias

    core = lax.rem(group, 2)
    near, far = 2 + 2 * core, 4 - 2 * core
    own_slots = [jnp.bitwise_xor(group, mask) for mask in (0, near, far, 6)]
    other_slots = [jnp.bitwise_xor(group, mask) for mask in (1, far + 1, near + 1, 7)]

    for chip in range(chips):
        for side, source in enumerate((tower_own_refs[chip], tower_other_refs[chip])):
            slot = jnp.bitwise_xor(group, 2 * chip + side)
            depth = source.shape[0]
            tower_full[pl.ds(pl.multiple_of(slot * depth, depth), depth), :] = source[...]

    for layer in range(layers):
        down_full[layer, pl.ds(base, block), :] = down_ref[layer]
        up_full[layer, pl.ds(base, block), :] = up_ref[layer]
        first = 2 * layer * slice_rows
        for step in range(1, members):
            owner = jnp.bitwise_xor(member, step)
            for chip in range(chips):
                for slots, sources in ((own_slots, own_refs), (other_slots, other_refs)):
                    source, slot = sources[chip], slots[chip]
                    at = pl.multiple_of(owner * block + slot * slice_rows, slice_rows)
                    down_full[layer, pl.ds(at, slice_rows), :] = source[
                        step - 1, first : first + slice_rows
                    ]
                    up_full[layer, pl.ds(at, slice_rows), :] = source[
                        step - 1, first + slice_rows : first + 2 * slice_rows
                    ]

    embedded = embedded_ref[...]
    crossed = embedded
    for layer in range(layers):
        projected = jnp.dot(
            crossed, down_full[layer], preferred_element_type=jnp.float32
        ).astype(jnp.bfloat16)
        lifted = lax.dot_general(
            projected,
            up_full[layer],
            (((1,), (1,)), ((), ())),
            preferred_element_type=jnp.float32,
        )
        crossed = (
            embedded.astype(jnp.float32) * (lifted + bias_full[layer : layer + 1, :])
            + crossed.astype(jnp.float32)
        ).astype(jnp.bfloat16)

    pre_act = jnp.dot(crossed, tower_full[...], preferred_element_type=jnp.float32)
    hidden = jnp.maximum(pre_act + tower_bias_ref[...], 0.0).astype(jnp.bfloat16)
    for step in range(members):
        owner = jnp.bitwise_xor(member, step)
        hidden_ref[pl.ds(pl.multiple_of(owner * rows, rows), rows), :] = hidden[
            step * rows : (step + 1) * rows
        ]


def flip_over(value, axis, mask):
    count = lax.axis_size(axis)
    return lax.ppermute(value, axis, [(i, i ^ mask) for i in range(count)])


def by_role(value, axis, even_mask, odd_mask):
    count = lax.axis_size(axis)
    pairs = [(i, i ^ (even_mask if i % 2 == 0 else odd_mask)) for i in range(count)]
    return lax.ppermute(value, axis, pairs)


def spread(value):
    near = by_role(value, "dp", 2, 4)
    far = by_role(value, "dp", 4, 2)
    across = by_role(near, "dp", 4, 2)
    return [value, near, far, across]


def gather_body(
    feature_ids,
    tables,
    table_of_feature,
    cross_down,
    cross_up,
    cross_bias,
    tower_weight,
    tower_bias,
):
    groups = lax.axis_size("dp")
    members = lax.axis_size("mp")
    group = lax.axis_index("dp")
    _, batch, _ = feature_ids.shape
    rows = batch // (groups * members)
    _, vocab, embed = tables.shape
    layers, block, rank = cross_down.shape
    width = block * members
    slice_rows = block // groups
    chips = groups // 2
    steps = range(1, members)

    down_slice = lax.dynamic_slice_in_dim(cross_down, group * slice_rows, slice_rows, 1)
    up_slice = lax.dynamic_slice_in_dim(cross_up, group * slice_rows, slice_rows, 1)
    matrices = []
    for layer in range(layers):
        matrices += [down_slice[layer], up_slice[layer]]
    payload = jnp.concatenate(matrices)
    legs = [flip_over(payload, "mp", step) for step in steps]

    bias_rows = -(-3 * cross_bias.size // embed // SUBLANES) * SUBLANES

    keep, send, terms = pl.pallas_call(
        functools.partial(pool_kernel, 256),
        out_shape=[jax.ShapeDtypeStruct((chips, rows, embed), jnp.bfloat16)] * 2
        + [jax.ShapeDtypeStruct((bias_rows, embed), jnp.bfloat16)],
        in_specs=[VMEM, VMEM, VMEM],
        out_specs=[VMEM] * 3,
        compiler_params=params(16),
        cost_estimate=pl.CostEstimate(
            flops=4 * vocab * groups * rows * embed, bytes_accessed=2**21, transcendentals=0
        ),
        name="pool",
    )(feature_ids[0].T, cross_bias, tables[0])
    crossing = flip_over(send, "dp", 1)
    both = jnp.stack([keep, crossing], axis=1)
    held = [both[0]] + [flip_over(both[chip], "dp", 2 * chip) for chip in range(1, chips)]
    piece = jnp.concatenate([part.reshape(-1, embed) for part in held] + [terms])

    got = jnp.stack([leg for leg in legs])
    own = spread(got)
    other = [flip_over(own[chip], "dp", 1) for chip in range(chips)]
    pieces = [piece] + [flip_over(piece, "mp", step) for step in steps]

    tower_own = [tower_weight] + [
        flip_over(tower_weight, "dp", 2 * chip) for chip in range(1, chips)
    ]
    tower_other = [flip_over(tower_own[chip], "dp", 1) for chip in range(chips)]

    samples = rows * members
    units = tower_weight.shape[1]
    inputs = [table_of_feature, cross_down, cross_up]
    inputs += [tower_bias.reshape(1, units)]
    inputs += own + other + tower_own + tower_other + pieces
    return pl.pallas_call(
        functools.partial(cross_kernel, members, chips),
        out_shape=jax.ShapeDtypeStruct((samples, units), jnp.bfloat16),
        in_specs=[SMEM] + [VMEM] * (len(inputs) - 1),
        out_specs=VMEM,
        scratch_shapes=[
            pltpu.VMEM((samples, width), jnp.bfloat16),
            pltpu.VMEM((layers, width), jnp.float32),
            pltpu.VMEM((layers, width, rank), jnp.bfloat16),
            pltpu.VMEM((layers, width, rank), jnp.bfloat16),
            pltpu.VMEM((width, units), jnp.bfloat16),
        ],
        compiler_params=params(32),
        cost_estimate=pl.CostEstimate(
            flops=2 * samples * width * (2 * layers * rank + units),
            bytes_accessed=2**23,
            transcendentals=0,
        ),
        name="cross",
    )(*inputs)


def solution(mesh):
    groups, members = mesh.shape["dp"], mesh.shape["mp"]

    def body(*args):
        feature_ids, tables, cross_down = args[0], args[1], args[3]
        _, block, _ = cross_down.shape
        rows = feature_ids.shape[1] // (groups * members)
        fits = 4 * cross_down.size * members <= GATHER_LIMIT
        fits = fits and block % tables.shape[2] == 0 and block % (SUBLANES * groups) == 0
        fits = fits and (rows == LANES // 2 or rows % LANES == 0) and groups == 2 * PLANE and members & (members - 1) == 0
        return (gather_body if fits else reduce_body)(*args)

    return jax.shard_map(
        body,
        mesh=mesh,
        in_specs=(
            P("dp", None, None),
            P("dp", None, None),
            P(),
            P(None, "mp", None),
            P(None, "mp", None),
            P(None, "mp"),
            P("dp", "mp"),
            P("mp"),
        ),
        out_specs=P("dp", "mp"),
        check_vma=False,
    )
```

```python
import functools

import jax
import jax.numpy as jnp
from jax import lax
from jax.experimental import pallas as pl
from jax.experimental.pallas import tpu as pltpu
from jax.sharding import PartitionSpec as P


GATHER_LIMIT = 12 * 2**20

LANES = 128
SUBLANES = 16
CHUNK = 256
PLANE = 4

VMEM = pl.BlockSpec(memory_space=pltpu.VMEM)
SMEM = pl.BlockSpec(memory_space=pltpu.SMEM)


def reduce_body(
    feature_ids,
    tables,
    table_of_feature,
    cross_down,
    cross_up,
    cross_bias,
    tower_weight,
    tower_bias,
):
    groups = lax.axis_size("dp")
    members = lax.axis_size("mp")
    member = lax.axis_index("mp")
    _, batch_size, hot_count = feature_ids.shape
    row_count = batch_size // (groups * members)
    shaped = feature_ids[0].reshape(groups, members, row_count, hot_count)
    own_ids = lax.dynamic_index_in_dim(shaped, member, 1, keepdims=False).reshape(
        groups * row_count, hot_count
    )
    summed = jnp.zeros((groups * row_count, tables.shape[2]), jnp.float32)
    for hot_index in range(hot_count):
        summed = summed + jnp.take(tables[0], own_ids[:, hot_index], axis=0).astype(jnp.float32)
    columns = [summed.astype(jnp.bfloat16)]
    pooled = jnp.stack(columns, axis=1)
    regrouped = lax.all_to_all(pooled, "dp", split_axis=0, concat_axis=1, tiled=True)
    ordered = jnp.take(regrouped, table_of_feature, axis=1)
    by_width = lax.all_to_all(ordered, "mp", split_axis=1, concat_axis=0, tiled=True)
    group_rows = by_width.shape[0]
    embedded = by_width.reshape(group_rows, -1)
    embedded_wide = embedded.astype(jnp.float32)
    crossed = embedded
    layer_total = cross_down.shape[0]
    for layer_index in range(layer_total):
        partial_value = jnp.dot(
            crossed, cross_down[layer_index], preferred_element_type=jnp.float32
        )
        projected = lax.psum(partial_value.astype(jnp.bfloat16), "mp")
        lifted = lax.dot_general(
            projected,
            cross_up[layer_index],
            (((1,), (1,)), ((), ())),
            preferred_element_type=jnp.float32,
        )
        crossed = (
            embedded_wide * (lifted + cross_bias[layer_index]) + crossed.astype(jnp.float32)
        ).astype(jnp.bfloat16)
    full_rows = lax.all_gather(crossed, "mp", axis=1, tiled=True)
    pre_act = jnp.dot(
        full_rows,
        lax.all_gather(tower_weight, "dp", axis=0, tiled=True),
        preferred_element_type=jnp.float32,
    )
    return jax.nn.relu(pre_act + tower_bias).astype(jnp.bfloat16)


def params(mib):
    return pltpu.CompilerParams(vmem_limit_bytes=mib * 2**20)


def select_kernel(groups, ids_ref, own_ref):
    batch = ids_ref.shape[1]
    rows = own_ref.shape[1] // groups
    per_group = batch // groups
    member = lax.axis_index("mp")
    wanted = []
    for owner in range(groups):
        if rows == LANES // 2:
            at = pl.multiple_of(owner * per_group + lax.div(member, 2) * LANES, LANES)
            wide = ids_ref[:, pl.ds(at, LANES)]
            wanted.append(jnp.where(lax.rem(member, 2) == 0, wide[:, :rows], wide[:, rows:]))
        else:
            at = pl.multiple_of(owner * per_group + member * rows, LANES)
            wanted.append(ids_ref[:, pl.ds(at, rows)])
    own_ref[...] = jnp.concatenate(wanted, axis=1)


def pool_kernel(
    chunk, ids_ref, bias_ref, table_ref, keep_ref, send_ref, terms_ref, marks_ref
):
    vocab, embed = table_ref.shape
    rest = bias_ref[...]
    layers, block = rest.shape
    parts = block // embed
    terms_ref[...] = jnp.zeros_like(terms_ref)
    for term in range(3):
        rounded = rest.astype(jnp.bfloat16)
        for layer in range(layers):
            for part in range(parts):
                terms_ref[pl.ds((term * layers + layer) * parts + part, 1), :] = rounded[
                    layer : layer + 1, part * embed : (part + 1) * embed
                ]
        rest = rest - rounded.astype(jnp.float32)
    hots = ids_ref.shape[0]
    chips, rows, _ = keep_ref.shape
    groups = 2 * chips
    samples = groups * rows
    group = lax.axis_index("dp")
    ids = ids_ref[...]
    total = jnp.zeros((embed, samples), jnp.float32)
    row_at = lax.broadcasted_iota(jnp.int16, (chunk, samples), 0)
    one = jnp.ones((), jnp.bfloat16)
    zero = jnp.zeros((), jnp.bfloat16)
    low = (ids & (chunk - 1)).astype(jnp.int16)
    high = lax.shift_right_logical(ids, chunk.bit_length() - 1)
    for hot in range(hots):
        marks_ref[hot] = jnp.where(low[hot : hot + 1, :] == row_at, one, zero)
    for start in range(0, vocab, chunk):
        inside = jnp.where(high == start // chunk, 1.0, 0.0).astype(jnp.bfloat16)
        counts = None
        for hot in range(hots):
            term = marks_ref[hot] * inside[hot : hot + 1, :]
            counts = term if counts is None else counts + term
        total = total + lax.dot_general(
            table_ref[start : start + chunk, :],
            counts,
            (((0,), (0,)), ((), ())),
            preferred_element_type=jnp.float32,
        )
    pooled = total.T.astype(jnp.bfloat16)
    core = lax.rem(group, 2)
    half = lax.div(group, 2)
    for chip in range(chips):
        at = jnp.bitwise_xor(half, chip)
        low = pooled[2 * chip * rows : (2 * chip + 1) * rows]
        high = pooled[(2 * chip + 1) * rows : (2 * chip + 2) * rows]
        keep_ref[at] = jnp.where(core == 0, low, high)
        send_ref[at] = jnp.where(core == 0, high, low)


def cross_kernel(members, chips, *refs):
    refs = list(refs)

    def take(count):
        taken = refs[:count]
        del refs[:count]
        return taken

    order_ref, down_ref, up_ref, tower_bias_ref = take(4)
    own_refs, other_refs = take(chips), take(chips)
    tower_own_refs, tower_other_refs = take(chips), take(chips)
    piece_refs = take(members)
    (hidden_ref,) = take(1)
    embedded_ref, bias_full, down_full, up_full, tower_full = take(5)

    group, member = lax.axis_index("dp"), lax.axis_index("mp")
    layers, block, _ = down_ref.shape
    tables = order_ref.shape[0]
    rows = hidden_ref.shape[0] // members
    embed = piece_refs[0].shape[1]
    slice_rows = block // (2 * chips)

    for feature in range(tables):
        slot = jnp.bitwise_xor(order_ref[feature], group)
        for step in range(members):
            embedded_ref[
                step * rows : (step + 1) * rows, feature * embed : (feature + 1) * embed
            ] = piece_refs[step][pl.ds(pl.multiple_of(slot * rows, rows), rows), :]

    base = pl.multiple_of(member * block, block)
    for step in range(members):
        owner = jnp.bitwise_xor(member, step)
        for layer in range(layers):
            for part in range(block // embed):
                at = tables * rows + (layer * block) // embed + part
                count = layers * block // embed
                bias = sum(
                    piece_refs[step][at + term * count, :].astype(jnp.float32).reshape(1, embed)
                    for term in range(3)
                )
                lane = pl.multiple_of(owner * block + part * embed, embed)
                bias_full[layer : layer + 1, pl.ds(lane, embed)] = bias

    core = lax.rem(group, 2)
    near, far = 2 + 2 * core, 4 - 2 * core
    own_slots = [jnp.bitwise_xor(group, mask) for mask in (0, near, far, 6)]
    other_slots = [jnp.bitwise_xor(group, mask) for mask in (1, far + 1, near + 1, 7)]

    for chip in range(chips):
        for side, source in enumerate((tower_own_refs[chip], tower_other_refs[chip])):
            slot = jnp.bitwise_xor(group, 2 * chip + side)
            depth = source.shape[0]
            tower_full[pl.ds(pl.multiple_of(slot * depth, depth), depth), :] = source[...]

    for layer in range(layers):
        down_full[layer, pl.ds(base, block), :] = down_ref[layer]
        up_full[layer, pl.ds(base, block), :] = up_ref[layer]
        first = 2 * layer * slice_rows
        for step in range(1, members):
            owner = jnp.bitwise_xor(member, step)
            for chip in range(chips):
                for slots, sources in ((own_slots, own_refs), (other_slots, other_refs)):
                    source, slot = sources[chip], slots[chip]
                    at = pl.multiple_of(owner * block + slot * slice_rows, slice_rows)
                    down_full[layer, pl.ds(at, slice_rows), :] = source[
                        step - 1, first : first + slice_rows
                    ]
                    up_full[layer, pl.ds(at, slice_rows), :] = source[
                        step - 1, first + slice_rows : first + 2 * slice_rows
                    ]

    embedded = embedded_ref[...]
    crossed = embedded
    for layer in range(layers):
        projected = jnp.dot(
            crossed, down_full[layer], preferred_element_type=jnp.float32
        ).astype(jnp.bfloat16)
        lifted = lax.dot_general(
            projected,
            up_full[layer],
            (((1,), (1,)), ((), ())),
            preferred_element_type=jnp.float32,
        )
        crossed = (
            embedded.astype(jnp.float32) * (lifted + bias_full[layer : layer + 1, :])
            + crossed.astype(jnp.float32)
        ).astype(jnp.bfloat16)

    pre_act = jnp.dot(crossed, tower_full[...], preferred_element_type=jnp.float32)
    hidden = jnp.maximum(pre_act + tower_bias_ref[...], 0.0).astype(jnp.bfloat16)
    for step in range(members):
        owner = jnp.bitwise_xor(member, step)
        hidden_ref[pl.ds(pl.multiple_of(owner * rows, rows), rows), :] = hidden[
            step * rows : (step + 1) * rows
        ]


def flip_over(value, axis, mask):
    count = lax.axis_size(axis)
    return lax.ppermute(value, axis, [(i, i ^ mask) for i in range(count)])


def by_role(value, axis, even_mask, odd_mask):
    count = lax.axis_size(axis)
    pairs = [(i, i ^ (even_mask if i % 2 == 0 else odd_mask)) for i in range(count)]
    return lax.ppermute(value, axis, pairs)


def spread(value):
    near = by_role(value, "dp", 2, 4)
    far = by_role(value, "dp", 4, 2)
    across = by_role(near, "dp", 4, 2)
    return [value, near, far, across]


def gather_body(
    feature_ids,
    tables,
    table_of_feature,
    cross_down,
    cross_up,
    cross_bias,
    tower_weight,
    tower_bias,
):
    groups = lax.axis_size("dp")
    members = lax.axis_size("mp")
    group = lax.axis_index("dp")
    _, batch, hots = feature_ids.shape
    rows = batch // (groups * members)
    _, vocab, embed = tables.shape
    layers, block, rank = cross_down.shape
    width = block * members
    slice_rows = block // groups
    chips = groups // 2
    steps = range(1, members)

    down_slice = lax.dynamic_slice_in_dim(cross_down, group * slice_rows, slice_rows, 1)
    up_slice = lax.dynamic_slice_in_dim(cross_up, group * slice_rows, slice_rows, 1)
    matrices = []
    for layer in range(layers):
        matrices += [down_slice[layer], up_slice[layer]]
    payload = jnp.concatenate(matrices)
    legs = [flip_over(payload, "mp", step) for step in steps]

    bias_rows = -(-3 * cross_bias.size // embed // SUBLANES) * SUBLANES

    own_ids = pl.pallas_call(
        functools.partial(select_kernel, groups),
        out_shape=jax.ShapeDtypeStruct((hots, groups * rows), jnp.int32),
        in_specs=[VMEM],
        out_specs=VMEM,
        compiler_params=params(2),
        cost_estimate=pl.CostEstimate(
            flops=4 * 10**9, bytes_accessed=2**17, transcendentals=0
        ),
        name="select",
    )(feature_ids[0].T)
    keep, send, terms = pl.pallas_call(
        functools.partial(pool_kernel, CHUNK),
        out_shape=[jax.ShapeDtypeStruct((chips, rows, embed), jnp.bfloat16)] * 2
        + [jax.ShapeDtypeStruct((bias_rows, embed), jnp.bfloat16)],
        in_specs=[VMEM, VMEM, VMEM],
        out_specs=[VMEM] * 3,
        scratch_shapes=[pltpu.VMEM((hots, CHUNK, groups * rows), jnp.bfloat16)],
        compiler_params=params(16),
        cost_estimate=pl.CostEstimate(
            flops=4 * vocab * groups * rows * embed, bytes_accessed=2**21, transcendentals=0
        ),
        name="pool",
    )(own_ids, cross_bias, tables[0])
    crossing = flip_over(send, "dp", 1)
    both = jnp.stack([keep, crossing], axis=1)
    held = [both[0]] + [flip_over(both[chip], "dp", 2 * chip) for chip in range(1, chips)]
    piece = jnp.concatenate([part.reshape(-1, embed) for part in held] + [terms])

    got = jnp.stack([leg for leg in legs])
    own = spread(got)
    other = [flip_over(own[chip], "dp", 1) for chip in range(chips)]
    pieces = [piece] + [flip_over(piece, "mp", step) for step in steps]

    tower_own = [tower_weight] + [
        flip_over(tower_weight, "dp", 2 * chip) for chip in range(1, chips)
    ]
    tower_other = [flip_over(tower_own[chip], "dp", 1) for chip in range(chips)]

    samples = rows * members
    units = tower_weight.shape[1]
    inputs = [table_of_feature, cross_down, cross_up]
    inputs += [tower_bias.reshape(1, units)]
    inputs += own + other + tower_own + tower_other + pieces
    return pl.pallas_call(
        functools.partial(cross_kernel, members, chips),
        out_shape=jax.ShapeDtypeStruct((samples, units), jnp.bfloat16),
        in_specs=[SMEM] + [VMEM] * (len(inputs) - 1),
        out_specs=VMEM,
        scratch_shapes=[
            pltpu.VMEM((samples, width), jnp.bfloat16),
            pltpu.VMEM((layers, width), jnp.float32),
            pltpu.VMEM((layers, width, rank), jnp.bfloat16),
            pltpu.VMEM((layers, width, rank), jnp.bfloat16),
            pltpu.VMEM((width, units), jnp.bfloat16),
        ],
        compiler_params=params(32),
        cost_estimate=pl.CostEstimate(
            flops=2 * samples * width * (2 * layers * rank + units),
            bytes_accessed=2**23,
            transcendentals=0,
        ),
        name="cross",
    )(*inputs)


def solution(mesh):
    groups, members = mesh.shape["dp"], mesh.shape["mp"]

    def body(*args):
        feature_ids, tables, cross_down = args[0], args[1], args[3]
        _, block, _ = cross_down.shape
        rows = feature_ids.shape[1] // (groups * members)
        fits = 4 * cross_down.size * members <= GATHER_LIMIT
        fits = fits and block % tables.shape[2] == 0 and block % (SUBLANES * groups) == 0
        fits = fits and (rows == LANES // 2 or rows % LANES == 0) and groups == 2 * PLANE and tables.shape[1] % CHUNK == 0 and members & (members - 1) == 0
        return (gather_body if fits else reduce_body)(*args)

    return jax.shard_map(
        body,
        mesh=mesh,
        in_specs=(
            P("dp", None, None),
            P("dp", None, None),
            P(),
            P(None, "mp", None),
            P(None, "mp", None),
            P(None, "mp"),
            P("dp", "mp"),
            P("mp"),
        ),
        out_specs=P("dp", "mp"),
        check_vma=False,
    )
```

```python
import functools

import jax
import jax.numpy as jnp
from jax import lax
from jax.experimental import pallas as pl
from jax.experimental.pallas import tpu as pltpu
from jax.sharding import PartitionSpec as P


GATHER_LIMIT = 12 * 2**20

LANES = 128
SUBLANES = 16
CHUNK = 256
PLANE = 4

VMEM = pl.BlockSpec(memory_space=pltpu.VMEM)
SMEM = pl.BlockSpec(memory_space=pltpu.SMEM)


def reduce_body(
    feature_ids,
    tables,
    table_of_feature,
    cross_down,
    cross_up,
    cross_bias,
    tower_weight,
    tower_bias,
):
    groups = lax.axis_size("dp")
    members = lax.axis_size("mp")
    member = lax.axis_index("mp")
    _, batch_size, hot_count = feature_ids.shape
    row_count = batch_size // (groups * members)
    shaped = feature_ids[0].reshape(groups, members, row_count, hot_count)
    own_ids = lax.dynamic_index_in_dim(shaped, member, 1, keepdims=False).reshape(
        groups * row_count, hot_count
    )
    summed = jnp.zeros((groups * row_count, tables.shape[2]), jnp.float32)
    for hot_index in range(hot_count):
        summed = summed + jnp.take(tables[0], own_ids[:, hot_index], axis=0).astype(jnp.float32)
    columns = [summed.astype(jnp.bfloat16)]
    pooled = jnp.stack(columns, axis=1)
    regrouped = lax.all_to_all(pooled, "dp", split_axis=0, concat_axis=1, tiled=True)
    ordered = jnp.take(regrouped, table_of_feature, axis=1)
    by_width = lax.all_to_all(ordered, "mp", split_axis=1, concat_axis=0, tiled=True)
    group_rows = by_width.shape[0]
    embedded = by_width.reshape(group_rows, -1)
    embedded_wide = embedded.astype(jnp.float32)
    crossed = embedded
    layer_total = cross_down.shape[0]
    for layer_index in range(layer_total):
        partial_value = jnp.dot(
            crossed, cross_down[layer_index], preferred_element_type=jnp.float32
        )
        projected = lax.psum(partial_value.astype(jnp.bfloat16), "mp")
        lifted = lax.dot_general(
            projected,
            cross_up[layer_index],
            (((1,), (1,)), ((), ())),
            preferred_element_type=jnp.float32,
        )
        crossed = (
            embedded_wide * (lifted + cross_bias[layer_index]) + crossed.astype(jnp.float32)
        ).astype(jnp.bfloat16)
    full_rows = lax.all_gather(crossed, "mp", axis=1, tiled=True)
    pre_act = jnp.dot(
        full_rows,
        lax.all_gather(tower_weight, "dp", axis=0, tiled=True),
        preferred_element_type=jnp.float32,
    )
    return jax.nn.relu(pre_act + tower_bias).astype(jnp.bfloat16)


def params(mib):
    return pltpu.CompilerParams(vmem_limit_bytes=mib * 2**20)


def select_kernel(groups, ids_ref, own_ref):
    batch = ids_ref.shape[1]
    rows = own_ref.shape[1] // groups
    per_group = batch // groups
    member = lax.axis_index("mp")
    wanted = []
    for owner in range(groups):
        if rows == LANES // 2:
            at = pl.multiple_of(owner * per_group + lax.div(member, 2) * LANES, LANES)
            wide = ids_ref[:, pl.ds(at, LANES)]
            wanted.append(jnp.where(lax.rem(member, 2) == 0, wide[:, :rows], wide[:, rows:]))
        else:
            at = pl.multiple_of(owner * per_group + member * rows, LANES)
            wanted.append(ids_ref[:, pl.ds(at, rows)])
    own_ref[...] = jnp.concatenate(wanted, axis=1)


def pool_kernel(
    chunk, ids_ref, bias_ref, table_ref, keep_ref, send_ref, terms_ref, marks_ref
):
    vocab, embed = table_ref.shape
    rest = bias_ref[...]
    layers, block = rest.shape
    parts = block // embed
    terms_ref[...] = jnp.zeros_like(terms_ref)
    for term in range(3):
        rounded = rest.astype(jnp.bfloat16)
        for layer in range(layers):
            for part in range(parts):
                terms_ref[pl.ds((term * layers + layer) * parts + part, 1), :] = rounded[
                    layer : layer + 1, part * embed : (part + 1) * embed
                ]
        rest = rest - rounded.astype(jnp.float32)
    hots = ids_ref.shape[0]
    chips, rows, _ = keep_ref.shape
    groups = 2 * chips
    samples = groups * rows
    group = lax.axis_index("dp")
    ids = ids_ref[...]
    total = jnp.zeros((embed, samples), jnp.float32)
    row_at = lax.broadcasted_iota(jnp.int16, (chunk, samples), 0)
    one = jnp.ones((), jnp.bfloat16)
    zero = jnp.zeros((), jnp.bfloat16)
    low = (ids & (chunk - 1)).astype(jnp.int16)
    high = lax.shift_right_logical(ids, chunk.bit_length() - 1)
    for hot in range(hots):
        marks_ref[hot] = jnp.where(low[hot : hot + 1, :] == row_at, one, zero)
    for start in range(0, vocab, chunk):
        inside = jnp.where(high == start // chunk, 1.0, 0.0).astype(jnp.bfloat16)
        counts = None
        for hot in range(hots):
            term = marks_ref[hot] * inside[hot : hot + 1, :]
            counts = term if counts is None else counts + term
        total = total + lax.dot_general(
            table_ref[start : start + chunk, :],
            counts,
            (((0,), (0,)), ((), ())),
            preferred_element_type=jnp.float32,
        )
    pooled = total.T.astype(jnp.bfloat16)
    core = lax.rem(group, 2)
    half = lax.div(group, 2)
    for chip in range(chips):
        at = jnp.bitwise_xor(half, chip)
        low = pooled[2 * chip * rows : (2 * chip + 1) * rows]
        high = pooled[(2 * chip + 1) * rows : (2 * chip + 2) * rows]
        keep_ref[at] = jnp.where(core == 0, low, high)
        send_ref[at] = jnp.where(core == 0, high, low)


def cross_kernel(members, chips, *refs):
    refs = list(refs)

    def take(count):
        taken = refs[:count]
        del refs[:count]
        return taken

    order_ref, down_ref, up_ref, tower_bias_ref = take(4)
    own_refs, other_refs = take(chips), take(chips)
    tower_own_refs, tower_other_refs = take(chips), take(chips)
    piece_refs = take(members)
    (hidden_ref,) = take(1)
    embedded_ref, bias_full, down_full, up_full, tower_full, done_ref, written = take(7)

    group, member = lax.axis_index("dp"), lax.axis_index("mp")
    layers, block, _ = down_ref.shape
    tables = order_ref.shape[0]
    rows = hidden_ref.shape[0] // members
    embed = piece_refs[0].shape[1]
    slice_rows = block // (2 * chips)

    for feature in range(tables):
        slot = jnp.bitwise_xor(order_ref[feature], group)
        for step in range(members):
            embedded_ref[
                step * rows : (step + 1) * rows, feature * embed : (feature + 1) * embed
            ] = piece_refs[step][pl.ds(pl.multiple_of(slot * rows, rows), rows), :]

    base = pl.multiple_of(member * block, block)
    for step in range(members):
        owner = jnp.bitwise_xor(member, step)
        for layer in range(layers):
            for part in range(block // embed):
                at = tables * rows + (layer * block) // embed + part
                count = layers * block // embed
                bias = sum(
                    piece_refs[step][at + term * count, :].astype(jnp.float32).reshape(1, embed)
                    for term in range(3)
                )
                lane = pl.multiple_of(owner * block + part * embed, embed)
                bias_full[layer : layer + 1, pl.ds(lane, embed)] = bias

    core = lax.rem(group, 2)
    near, far = 2 + 2 * core, 4 - 2 * core
    own_slots = [jnp.bitwise_xor(group, mask) for mask in (0, near, far, 6)]
    other_slots = [jnp.bitwise_xor(group, mask) for mask in (1, far + 1, near + 1, 7)]

    embedded = embedded_ref[...]
    crossed = embedded
    for layer in range(layers):
        down_full[layer, pl.ds(base, block), :] = down_ref[layer]
        up_full[layer, pl.ds(base, block), :] = up_ref[layer]
        first = 2 * layer * slice_rows
        for step in range(1, members):
            owner = jnp.bitwise_xor(member, step)
            for chip in range(chips):
                for slots, sources in ((own_slots, own_refs), (other_slots, other_refs)):
                    source, slot = sources[chip], slots[chip]
                    at = pl.multiple_of(owner * block + slot * slice_rows, slice_rows)
                    down_full[layer, pl.ds(at, slice_rows), :] = source[
                        step - 1, first : first + slice_rows
                    ]
                    up_full[layer, pl.ds(at, slice_rows), :] = source[
                        step - 1, first + slice_rows : first + 2 * slice_rows
                    ]
        projected = jnp.dot(
            crossed, down_full[layer], preferred_element_type=jnp.float32
        ).astype(jnp.bfloat16)
        lifted = lax.dot_general(
            projected,
            up_full[layer],
            (((1,), (1,)), ((), ())),
            preferred_element_type=jnp.float32,
        )
        crossed = (
            embedded.astype(jnp.float32) * (lifted + bias_full[layer : layer + 1, :])
            + crossed.astype(jnp.float32)
        ).astype(jnp.bfloat16)

    for chip in range(chips):
        for side, source in enumerate((tower_own_refs[chip], tower_other_refs[chip])):
            slot = jnp.bitwise_xor(group, 2 * chip + side)
            depth = source.shape[0]
            tower_full[pl.ds(pl.multiple_of(slot * depth, depth), depth), :] = source[...]
    units = tower_full.shape[1]
    part = units // 2
    copies = []
    for index in range(2):
        columns = slice(index * part, (index + 1) * part)
        pre_act = jnp.dot(crossed, tower_full[:, columns], preferred_element_type=jnp.float32)
        hidden = jnp.maximum(pre_act + tower_bias_ref[:, columns], 0.0).astype(jnp.bfloat16)
        for step in range(members):
            owner = jnp.bitwise_xor(member, step)
            done_ref[index, pl.ds(pl.multiple_of(owner * rows, rows), rows), :] = hidden[
                step * rows : (step + 1) * rows
            ]
        copy = pltpu.make_async_copy(
            done_ref.at[index], hidden_ref.at[:, pl.ds(index * part, part)], written.at[index]
        )
        copy.start()
        copies.append(copy)
    for copy in copies:
        copy.wait()


def flip_over(value, axis, mask):
    count = lax.axis_size(axis)
    return lax.ppermute(value, axis, [(i, i ^ mask) for i in range(count)])


def by_role(value, axis, even_mask, odd_mask):
    count = lax.axis_size(axis)
    pairs = [(i, i ^ (even_mask if i % 2 == 0 else odd_mask)) for i in range(count)]
    return lax.ppermute(value, axis, pairs)


def spread(value):
    near = by_role(value, "dp", 2, 4)
    far = by_role(value, "dp", 4, 2)
    across = by_role(near, "dp", 4, 2)
    return [value, near, far, across]


def gather_body(
    feature_ids,
    tables,
    table_of_feature,
    cross_down,
    cross_up,
    cross_bias,
    tower_weight,
    tower_bias,
):
    groups = lax.axis_size("dp")
    members = lax.axis_size("mp")
    group = lax.axis_index("dp")
    _, batch, hots = feature_ids.shape
    rows = batch // (groups * members)
    _, vocab, embed = tables.shape
    layers, block, rank = cross_down.shape
    width = block * members
    slice_rows = block // groups
    chips = groups // 2
    steps = range(1, members)

    down_slice = lax.dynamic_slice_in_dim(cross_down, group * slice_rows, slice_rows, 1)
    up_slice = lax.dynamic_slice_in_dim(cross_up, group * slice_rows, slice_rows, 1)
    matrices = []
    for layer in range(layers):
        matrices += [down_slice[layer], up_slice[layer]]
    payload = jnp.concatenate(matrices)
    legs = [flip_over(payload, "mp", step) for step in steps]

    bias_rows = -(-3 * cross_bias.size // embed // SUBLANES) * SUBLANES

    own_ids = pl.pallas_call(
        functools.partial(select_kernel, groups),
        out_shape=jax.ShapeDtypeStruct((hots, groups * rows), jnp.int32),
        in_specs=[VMEM],
        out_specs=VMEM,
        compiler_params=params(2),
        cost_estimate=pl.CostEstimate(
            flops=4 * 10**9, bytes_accessed=2**17, transcendentals=0
        ),
        name="select",
    )(feature_ids[0].T)
    keep, send, terms = pl.pallas_call(
        functools.partial(pool_kernel, CHUNK),
        out_shape=[jax.ShapeDtypeStruct((chips, rows, embed), jnp.bfloat16)] * 2
        + [jax.ShapeDtypeStruct((bias_rows, embed), jnp.bfloat16)],
        in_specs=[VMEM, VMEM, VMEM],
        out_specs=[VMEM] * 3,
        scratch_shapes=[pltpu.VMEM((hots, CHUNK, groups * rows), jnp.bfloat16)],
        compiler_params=params(16),
        cost_estimate=pl.CostEstimate(
            flops=4 * vocab * groups * rows * embed, bytes_accessed=2**21, transcendentals=0
        ),
        name="pool",
    )(own_ids, cross_bias, tables[0])
    crossing = flip_over(send, "dp", 1)
    both = jnp.stack([keep, crossing], axis=1)
    held = [both[0]] + [flip_over(both[chip], "dp", 2 * chip) for chip in range(1, chips)]
    piece = jnp.concatenate([part.reshape(-1, embed) for part in held] + [terms])

    got = jnp.stack([leg for leg in legs])
    own = spread(got)
    other = [flip_over(own[chip], "dp", 1) for chip in range(chips)]
    pieces = [piece] + [flip_over(piece, "mp", step) for step in steps]

    tower_own = [tower_weight] + [
        flip_over(tower_weight, "dp", 2 * chip) for chip in range(1, chips)
    ]
    tower_other = [flip_over(tower_own[chip], "dp", 1) for chip in range(chips)]

    samples = rows * members
    units = tower_weight.shape[1]
    inputs = [table_of_feature, cross_down, cross_up]
    inputs += [tower_bias.reshape(1, units)]
    inputs += own + other + tower_own + tower_other + pieces
    return pl.pallas_call(
        functools.partial(cross_kernel, members, chips),
        out_shape=jax.ShapeDtypeStruct((samples, units), jnp.bfloat16),
        in_specs=[SMEM] + [VMEM] * (len(inputs) - 1),
        out_specs=pl.BlockSpec(memory_space=pl.ANY),
        scratch_shapes=[
            pltpu.VMEM((samples, width), jnp.bfloat16),
            pltpu.VMEM((layers, width), jnp.float32),
            pltpu.VMEM((layers, width, rank), jnp.bfloat16),
            pltpu.VMEM((layers, width, rank), jnp.bfloat16),
            pltpu.VMEM((width, units), jnp.bfloat16),
            pltpu.VMEM((2, samples, units // 2), jnp.bfloat16),
            pltpu.SemaphoreType.DMA((2,)),
        ],
        compiler_params=params(32),
        cost_estimate=pl.CostEstimate(
            flops=2 * samples * width * (2 * layers * rank + units),
            bytes_accessed=2**23,
            transcendentals=0,
        ),
        name="cross",
    )(*inputs)


def solution(mesh):
    groups, members = mesh.shape["dp"], mesh.shape["mp"]

    def body(*args):
        feature_ids, tables, cross_down = args[0], args[1], args[3]
        _, block, _ = cross_down.shape
        rows = feature_ids.shape[1] // (groups * members)
        fits = 4 * cross_down.size * members <= GATHER_LIMIT
        fits = fits and block % tables.shape[2] == 0 and block % (SUBLANES * groups) == 0
        fits = fits and (rows == LANES // 2 or rows % LANES == 0) and groups == 2 * PLANE and tables.shape[1] % CHUNK == 0 and members & (members - 1) == 0
        return (gather_body if fits else reduce_body)(*args)

    return jax.shard_map(
        body,
        mesh=mesh,
        in_specs=(
            P("dp", None, None),
            P("dp", None, None),
            P(),
            P(None, "mp", None),
            P(None, "mp", None),
            P(None, "mp"),
            P("dp", "mp"),
            P("mp"),
        ),
        out_specs=P("dp", "mp"),
        check_vma=False,
    )
```
